32 devices in a mesh: row: 8 (over z, x), col: 4 (over y, core).
Axes of the slice: x: 2, y: 2, z: 4, core: 2. Of those that a mesh axis runs over, the one named last changes fastest.
Arguments:
- old_params: float32 [2, 64, 131072], P(None, ('row', 'col')), may hold values from -0.12 to 0.12
- old_first: float32 [2, 64, 131072], P(None, ('row', 'col')), may hold values from -1.8 to 1.8
- old_second: float32 [2, 64, 131072], P(None, ('row', 'col')), may hold values from 0.001 to 1
- gradients: float32 [2, 32, 262144], P(None, ('row', 'col')), may hold values from -250 to 250
- old_table: int32 [2, 64], replicated, may hold values from 0 to 63, as said below
- new_table: int32 [2, 32], replicated, may hold values from 0 to 31, as said below
Outputs:
- new_params: float32 [2, 32, 262144], P(None, ('row', 'col'))
- new_first: float32 [2, 32, 262144], P(None, ('row', 'col'))
- new_second: float32 [2, 32, 262144], P(None, ('row', 'col'))
The draws below stay inside these ranges and needn't reach their ends.
Inputs may be any that keep to these rules, and one draw needn't show every extreme that they name: old_table[t, p] = p XOR k for one k per tensor. new_table[t, q] = q XOR k for one k per tensor.
All inputs are finite; a program needn't handle non-finite values.
Results may differ from the reference program's by a relative error of at most 0.00002.
Values sent between devices are 32-bit elements; how exact they have to be, the bound alone decides.
A program may use at most 64 MiB of HBM per device.

```python
import math
import jax
import jax.numpy as jnp

STEP = 100
NT = 2
ELEMS = 8388608
OLD_SHARDS = 64
OB = 131072
DEVICES = 32


def draw_old_table(key, part):
    folded = jax.random.fold_in(key, 11)
    offsets = jax.random.randint(folded, (NT, 1), 0, OLD_SHARDS)
    return jnp.bitwise_xor(jnp.arange(OLD_SHARDS, dtype=jnp.int32)[None, :], offsets).astype(jnp.int32)


def draw_new_table(key, part):
    folded = jax.random.fold_in(key, 23)
    offsets = jax.random.randint(folded, (NT, 1), 0, DEVICES)
    return jnp.bitwise_xor(jnp.arange(DEVICES, dtype=jnp.int32)[None, :], offsets).astype(jnp.int32)


def draw_gradients(key, part):
    folded = jax.random.fold_in(key, 37)
    key_private = jax.random.fold_in(folded, 0)
    position = jnp.arange(DEVICES, dtype=jnp.float32)[None, :, None]
    rising = 1.0 + 2.0 * position / max(DEVICES - 1, 1)
    private = jnp.clip(jax.random.normal(key_private, (NT, DEVICES, 2 * OB)), -8.0, 8.0)
    return (rising * private).astype(jnp.float32)


def shard_levels(own_key, shape, cuts, smallest, top_value):
    factor_of, own = 1.0, jax.random.fold_in(own_key, 6)
    for axis_at, parts in cuts:
        draws = jnp.exp(jax.random.uniform(jax.random.fold_in(own, axis_at), (parts,), jnp.float32, smallest / len(cuts), top_value / len(cuts)))
        factor_of = factor_of * jnp.repeat(draws, shape[axis_at] // parts).reshape([-1 if axis == axis_at else 1 for axis in range(len(shape))])
    return factor_of


def noise(key, shape, spread, most, cuts=(), held_as=jnp.bfloat16):
    gain = shard_levels(key, shape, cuts, -0.22, 0.18) if cuts else 1.0
    entries = jax.random.normal(key, shape, jnp.float32) * spread * gain
    return jnp.minimum(jnp.maximum(entries, -most), most).astype(held_as)


def setup_inputs(seed: int = 0) -> dict:
    seeds = jax.random.split(jax.random.key(seed), 7)
    return {
        "old_params": noise(seeds[0], (NT, OLD_SHARDS, OB), 0.02, 0.12, ((1, 32),), jnp.float32),
        "old_first": noise(seeds[1], (NT, OLD_SHARDS, OB), 0.3, 1.8, ((1, 32),), jnp.float32),
        "old_second": jnp.clip(jnp.exp(math.log(1.0) - 6.9077552 * jax.random.uniform(seeds[2], (NT, OLD_SHARDS, OB), jnp.float32) ** shard_levels(seeds[2], (NT, OLD_SHARDS, OB), ((1, 32),), -0.2, 0.2)), 0.001, 1.0),
        "gradients": draw_gradients(jax.random.fold_in(seeds[6], 71), 0),
        "old_table": draw_old_table(jax.random.fold_in(seeds[6], 71), 0),
        "new_table": draw_new_table(jax.random.fold_in(seeds[6], 71), 0),
    }


beta_one = 0.9
beta_two = 0.95
epsilon = 1e-08
learn_rate = 0.001
decay_rate = 0.1

def relayout(old_state, old_table, new_table):
    tensors = jnp.arange(old_state.shape[0], dtype=jnp.int32)[:, None]
    blocks = jnp.zeros_like(old_state).at[tensors, old_table].set(old_state)
    paired = blocks.reshape(old_state.shape[0], old_state.shape[1] // 2, 2 * old_state.shape[2])
    return paired[tensors, new_table]

def adam_update(params, first_moment, second_moment, gradients, clip_factor):
    scaled = clip_factor * gradients
    first_new = beta_one * first_moment + (1.0 - beta_one) * scaled
    second_new = beta_two * second_moment + (1.0 - beta_two) * scaled * scaled
    bias_first = 1.0 - beta_one ** STEP
    bias_second = 1.0 - beta_two ** STEP
    update = first_new / bias_first / (jnp.sqrt(second_new / bias_second) + epsilon)
    params_new = params - learn_rate * (update + decay_rate * params)
    return (params_new, first_new, second_new)

def reference(old_params, old_first, old_second, gradients, old_table, new_table):
    moved_params = relayout(old_params, old_table, new_table)
    moved_first = relayout(old_first, old_table, new_table)
    moved_second = relayout(old_second, old_table, new_table)
    grad_norm = jnp.sqrt(jnp.sum(gradients * gradients))
    limit = jnp.float32(0.5 * (NT * ELEMS) ** 0.5)
    clip_factor = limit / jnp.maximum(grad_norm, limit)
    return adam_update(moved_params, moved_first, moved_second, gradients, clip_factor)
```

```python
import functools
import math

import jax
import jax.numpy as jnp
from jax import lax
from jax.experimental import pallas as pl
from jax.experimental.pallas import tpu as pltpu
from jax.sharding import PartitionSpec as P

STEP = 100
LANES = 128
AXES = ("row", "col")
JOINT_DEVICES = 1


beta_one = 0.9
beta_two = 0.95
epsilon = 1e-08
learn_rate = 0.001
decay_rate = 0.1


def adam_update(params, first_moment, second_moment, gradients, clip_factor):
    scaled = clip_factor * gradients
    first_new = beta_one * first_moment + (1.0 - beta_one) * scaled
    second_new = beta_two * second_moment + (1.0 - beta_two) * scaled * scaled
    bias_first = 1.0 - beta_one**STEP
    bias_second = 1.0 - beta_two**STEP
    update = first_new / bias_first / (jnp.sqrt(second_new / bias_second) + epsilon)
    params_new = params - learn_rate * (update + decay_rate * params)
    return (params_new, first_new, second_new)


def pack_kernel(low_ref, params_ref, first_ref, second_ref, grad_ref, out_zero, out_one, squares_ref):
    for tensor, out_ref in enumerate((out_zero, out_one)):
        low_set = low_ref[tensor] == 1
        for number, state_ref in enumerate((params_ref, first_ref, second_ref)):
            even = state_ref[tensor, :, 0, :]
            odd = state_ref[tensor, :, 1, :]
            out_ref[number, 0] = jnp.where(low_set, odd, even)
            out_ref[number, 1] = jnp.where(low_set, even, odd)

    @pl.when(pl.program_id(0) == 0)
    def _():
        squares_ref[...] = jnp.zeros_like(squares_ref)

    grads = grad_ref[...]
    squares_ref[...] += jnp.sum((grads * grads).reshape(-1, 8, LANES), axis=0)


def pack(low_bits, old_params, old_first, old_second, gradients):
    tensors, halves, rows, lanes = gradients.shape
    step = min(rows, 128)
    state_spec = pl.BlockSpec((tensors, step, halves, lanes), lambda i: (0, i, 0, 0))
    out_spec = pl.BlockSpec((3, halves, step, lanes), lambda i: (0, 0, i, 0))
    packed = jax.ShapeDtypeStruct((3, halves, rows, lanes), jnp.float32)
    return pl.pallas_call(
        pack_kernel,
        grid=(rows // step,),
        in_specs=[
            pl.BlockSpec(memory_space=pltpu.SMEM),
            state_spec,
            state_spec,
            state_spec,
            pl.BlockSpec((tensors, halves, step, lanes), lambda i: (0, 0, i, 0)),
        ],
        out_specs=[out_spec, out_spec, pl.BlockSpec((8, lanes), lambda i: (0, 0))],
        out_shape=[packed, packed, jax.ShapeDtypeStruct((8, lanes), jnp.float32)],
    )(low_bits, old_params, old_first, old_second, gradients)


def update_kernel(clip_ref, zero_ref, one_ref, grad_ref, params_out, first_out, second_out):
    clip_factor = clip_ref[0]
    for tensor, moved_ref in enumerate((zero_ref, one_ref)):
        params, first, second = adam_update(
            moved_ref[0], moved_ref[1], moved_ref[2], grad_ref[tensor], clip_factor
        )
        params_out[tensor] = params
        first_out[tensor] = first
        second_out[tensor] = second


def update(clip_factor, zero, one, gradients):
    tensors, halves, rows, lanes = gradients.shape
    step = min(rows, 128)
    moved_spec = pl.BlockSpec((3, halves, step, lanes), lambda i: (0, 0, i, 0))
    flat_spec = pl.BlockSpec((tensors, halves, step, lanes), lambda i: (0, 0, i, 0))
    return pl.pallas_call(
        update_kernel,
        grid=(rows // step,),
        in_specs=[pl.BlockSpec(memory_space=pltpu.SMEM), moved_spec, moved_spec, flat_spec],
        out_specs=[flat_spec] * 3,
        out_shape=[jax.ShapeDtypeStruct(gradients.shape, jnp.float32)] * 3,
    )(clip_factor, zero, one, gradients)


def shift(array, key, devices):
    if key == 0:
        return array
    return lax.ppermute(array, AXES, [(i, i ^ key) for i in range(devices)])


def move_joint(zero, one, keys, devices):
    def branch(key_zero, key_one, arrays):
        return (shift(arrays[0], key_zero, devices), shift(arrays[1], key_one, devices))

    branches = [functools.partial(branch, i // devices, i % devices) for i in range(devices * devices)]
    return lax.switch(keys[0] * devices + keys[1], branches, (zero, one))


def move_each(zero, one, keys, devices):
    branches = [functools.partial(shift, key=i, devices=devices) for i in range(devices)]
    return (lax.switch(keys[0], branches, zero), lax.switch(keys[1], branches, one))


def shards(old_params, old_first, old_second, gradients, old_table, new_table):
    tensors, halves, width = old_params.shape
    devices = lax.axis_size(AXES)
    rows = width // LANES
    old_key = old_table[:, 0]
    keys = jnp.bitwise_xor(jnp.right_shift(old_key, 1), new_table[:, 0])
    low_bits = jnp.bitwise_and(old_key, 1)

    def paired(array):
        return array.reshape(tensors, halves, rows, LANES).transpose(0, 2, 1, 3)

    flat = gradients.reshape(tensors, halves, rows, LANES)
    zero, one, squares = pack(low_bits, paired(old_params), paired(old_first), paired(old_second), flat)
    total_squares = lax.psum(jnp.sum(squares), AXES)
    limit = jnp.float32(0.5 * math.sqrt(gradients.size * devices))
    clip_factor = limit / jnp.maximum(jnp.sqrt(total_squares), limit)
    move = move_joint if devices <= JOINT_DEVICES else move_each
    zero, one = move(zero, one, keys, devices)
    results = update(clip_factor.reshape(1), zero, one, flat)
    return tuple(result.reshape(gradients.shape) for result in results)


def solution(mesh):
    spec = P(None, AXES, None)
    return jax.shard_map(
        shards,
        mesh=mesh,
        in_specs=(spec, spec, spec, spec, P(), P()),
        out_specs=(spec, spec, spec),
        check_vma=False,
    )
```

```python
import functools
import math

import jax
import jax.numpy as jnp
from jax import lax
from jax.experimental import pallas as pl
from jax.experimental.pallas import tpu as pltpu
from jax.sharding import PartitionSpec as P

STEP = 100
LANES = 128
AXES = ("row", "col")
WIDE = 128
NARROW = 32


beta_one = 0.9
beta_two = 0.95
epsilon = 1e-08
learn_rate = 0.001
decay_rate = 0.1


def adam_update(params, first_moment, second_moment, gradients, clip_factor):
    scaled = clip_factor * gradients
    first_new = beta_one * first_moment + (1.0 - beta_one) * scaled
    second_new = beta_two * second_moment + (1.0 - beta_two) * scaled * scaled
    bias_first = 1.0 - beta_one**STEP
    bias_second = 1.0 - beta_two**STEP
    update = first_new / bias_first / (jnp.sqrt(second_new / bias_second) + epsilon)
    params_new = params - learn_rate * (update + decay_rate * params)
    return (params_new, first_new, second_new)


def pack_kernel(low_ref, params_ref, first_ref, second_ref, out_ref):
    low_set = low_ref[0] == 1
    for number, state_ref in enumerate((params_ref, first_ref, second_ref)):
        even = state_ref[0, :, 0, :]
        odd = state_ref[0, :, 1, :]
        out_ref[number, 0] = jnp.where(low_set, odd, even)
        out_ref[number, 1] = jnp.where(low_set, even, odd)


def pack(tensor, low_bit, old_params, old_first, old_second, most):
    tensors, rows, halves, lanes = old_params.shape
    step = min(rows, most)
    state_spec = pl.BlockSpec((1, step, halves, lanes), lambda i: (tensor, i, 0, 0))
    size = 3 * halves * rows * lanes
    return pl.pallas_call(
        pack_kernel,
        grid=(rows // step,),
        in_specs=[pl.BlockSpec(memory_space=pltpu.SMEM), state_spec, state_spec, state_spec],
        out_specs=pl.BlockSpec((3, halves, step, lanes), lambda i: (0, 0, i, 0)),
        out_shape=jax.ShapeDtypeStruct((3, halves, rows, lanes), jnp.float32),
        cost_estimate=pl.CostEstimate(flops=size, bytes_accessed=8 * size, transcendentals=0),
    )(low_bit, old_params, old_first, old_second)


def squares_kernel(grad_ref, squares_ref):
    @pl.when(pl.program_id(0) == 0)
    def _():
        squares_ref[...] = jnp.zeros_like(squares_ref)

    grads = grad_ref[...]
    squares_ref[...] += jnp.sum((grads * grads).reshape(-1, 8, LANES), axis=0)


def sum_squares(gradients):
    tensors, halves, rows, lanes = gradients.shape
    step = min(rows, NARROW)
    return pl.pallas_call(
        squares_kernel,
        grid=(rows // step,),
        in_specs=[pl.BlockSpec((tensors, halves, step, lanes), lambda i: (0, 0, i, 0))],
        out_specs=pl.BlockSpec((8, lanes), lambda i: (0, 0)),
        out_shape=jax.ShapeDtypeStruct((8, lanes), jnp.float32),
        cost_estimate=pl.CostEstimate(
            flops=2 * gradients.size, bytes_accessed=4 * gradients.size, transcendentals=0
        ),
    )(gradients)


def clip_kernel(limit, total_ref, clip_ref):
    total = jnp.full((8, LANES), total_ref[0], jnp.float32)
    clip_ref[...] = limit / jnp.maximum(jnp.sqrt(total), limit)


def clip_from(total_squares, limit):
    return pl.pallas_call(
        functools.partial(clip_kernel, limit),
        in_specs=[pl.BlockSpec(memory_space=pltpu.SMEM)],
        out_shape=jax.ShapeDtypeStruct((8, LANES), jnp.float32),
    )(total_squares.reshape(1))


def update_kernel(clip_ref, moved_ref, grad_ref, *refs):
    params_out, first_out, second_out = refs[-3:]
    params, first, second = adam_update(
        moved_ref[0], moved_ref[1], moved_ref[2], grad_ref[0], clip_ref[0, 0]
    )
    params_out[0] = params
    first_out[0] = first
    second_out[0] = second


def update(tensor, clip_factor, moved, gradients, most, filled=()):
    tensors, halves, rows, lanes = gradients.shape
    step = min(rows, most)
    flat_spec = pl.BlockSpec((1, halves, step, lanes), lambda i: (tensor, 0, i, 0))
    size = halves * rows * lanes
    return pl.pallas_call(
        update_kernel,
        grid=(rows // step,),
        in_specs=[
            pl.BlockSpec(memory_space=pltpu.SMEM),
            pl.BlockSpec((3, halves, step, lanes), lambda i: (0, 0, i, 0)),
            flat_spec,
        ]
        + [pl.BlockSpec(memory_space=pl.ANY)] * len(filled),
        out_specs=[flat_spec] * 3,
        out_shape=[jax.ShapeDtypeStruct(gradients.shape, jnp.float32)] * 3,
        input_output_aliases={3 + i: i for i in range(len(filled))},
        cost_estimate=pl.CostEstimate(flops=20 * size, bytes_accessed=28 * size, transcendentals=2 * size),
    )(clip_factor, moved, gradients, *filled)


def shift(array, key, devices):
    if key == 0:
        return array
    return lax.ppermute(array, AXES, [(i, i ^ key) for i in range(devices)])


def shards(old_params, old_first, old_second, gradients, old_table, new_table):
    tensors, halves, width = old_params.shape
    devices = lax.axis_size(AXES)
    rows = width // LANES
    old_key = old_table[:, 0]
    keys = jnp.bitwise_xor(jnp.right_shift(old_key, 1), new_table[:, 0])
    low_bits = jnp.bitwise_and(old_key, 1)

    def paired(array):
        return array.reshape(tensors, halves, rows, LANES).transpose(0, 2, 1, 3)

    flat = gradients.reshape(tensors, halves, rows, LANES)
    states = (paired(old_params), paired(old_first), paired(old_second))
    limit = 0.5 * math.sqrt(gradients.size * devices)

    def move_first(key, operands):
        zero, flat, low_bit, states = operands
        moved = shift(zero, key, devices)
        total_squares = lax.psum(jnp.sum(sum_squares(flat)), AXES)
        return (moved, pack(1, low_bit, *states, NARROW), clip_from(total_squares, limit))

    def move_second(key, operands):
        one, zero, flat, clip_factor = operands
        return (shift(one, key, devices), update(0, clip_factor, zero, flat, NARROW))

    def chosen(move, key, operands):
        return lax.switch(key, [functools.partial(move, i) for i in range(devices)], operands)

    zero = pack(0, low_bits[:1], *states, WIDE)
    zero, one, clip_factor = chosen(move_first, keys[0], (zero, flat, low_bits[1:], states))
    one, results = chosen(move_second, keys[1], (one, zero, flat, clip_factor))
    results = update(1, clip_factor, one, flat, WIDE, results)
    return tuple(result.reshape(gradients.shape) for result in results)


def solution(mesh):
    spec = P(None, AXES, None)
    return jax.shard_map(
        shards,
        mesh=mesh,
        in_specs=(spec, spec, spec, spec, P(), P()),
        out_specs=(spec, spec, spec),
        check_vma=False,
    )
```

```python
import functools
import math

import jax
import jax.numpy as jnp
from jax import lax
from jax.experimental import pallas as pl
from jax.experimental.pallas import tpu as pltpu
from jax.sharding import PartitionSpec as P

STEP = 100
LANES = 128
AXES = ("row", "col")
JOINT_DEVICES = 1


beta_one = 0.9
beta_two = 0.95
epsilon = 1e-08
learn_rate = 0.001
decay_rate = 0.1


def adam_update(params, first_moment, second_moment, gradients, clip_factor):
    scaled = clip_factor * gradients
    first_new = beta_one * first_moment + (1.0 - beta_one) * scaled
    second_new = beta_two * second_moment + (1.0 - beta_two) * scaled * scaled
    bias_first = 1.0 - beta_one**STEP
    bias_second = 1.0 - beta_two**STEP
    update = first_new / bias_first / (jnp.sqrt(second_new / bias_second) + epsilon)
    params_new = params - learn_rate * (update + decay_rate * params)
    return (params_new, first_new, second_new)


def pack_kernel(low_ref, params_ref, first_ref, second_ref, grad_ref, out_zero, out_one, squares_ref):
    for tensor, out_ref in enumerate((out_zero, out_one)):
        low_set = low_ref[tensor] == 1
        for number, state_ref in enumerate((params_ref, first_ref, second_ref)):
            even = state_ref[tensor, :, 0, :]
            odd = state_ref[tensor, :, 1, :]
            out_ref[number, 0] = jnp.where(low_set, odd, even)
            out_ref[number, 1] = jnp.where(low_set, even, odd)

    @pl.when(pl.program_id(0) == 0)
    def _():
        squares_ref[...] = jnp.zeros_like(squares_ref)

    grads = grad_ref[...]
    squares_ref[...] += jnp.sum((grads * grads).reshape(-1, 8, LANES), axis=0)


def pack(low_bits, old_params, old_first, old_second, gradients):
    tensors, halves, rows, lanes = gradients.shape
    step = min(rows, 128)
    state_spec = pl.BlockSpec((tensors, step, halves, lanes), lambda i: (0, i, 0, 0))
    out_spec = pl.BlockSpec((3, halves, step, lanes), lambda i: (0, 0, i, 0))
    packed = jax.ShapeDtypeStruct((3, halves, rows, lanes), jnp.float32)
    return pl.pallas_call(
        pack_kernel,
        grid=(rows // step,),
        in_specs=[
            pl.BlockSpec(memory_space=pltpu.SMEM),
            state_spec,
            state_spec,
            state_spec,
            pl.BlockSpec((tensors, halves, step, lanes), lambda i: (0, 0, i, 0)),
        ],
        out_specs=[out_spec, out_spec, pl.BlockSpec((8, lanes), lambda i: (0, 0))],
        out_shape=[packed, packed, jax.ShapeDtypeStruct((8, lanes), jnp.float32)],
    )(low_bits, old_params, old_first, old_second, gradients)


def update_kernel(clip_ref, zero_ref, one_ref, grad_ref, params_out, first_out, second_out):
    clip_factor = clip_ref[0]
    for tensor, moved_ref in enumerate((zero_ref, one_ref)):
        params, first, second = adam_update(
            moved_ref[0], moved_ref[1], moved_ref[2], grad_ref[tensor], clip_factor
        )
        params_out[tensor] = params
        first_out[tensor] = first
        second_out[tensor] = second


def update(clip_factor, zero, one, gradients):
    tensors, halves, rows, lanes = gradients.shape
    step = min(rows, 128)
    moved_spec = pl.BlockSpec((3, halves, step, lanes), lambda i: (0, 0, i, 0))
    flat_spec = pl.BlockSpec((tensors, halves, step, lanes), lambda i: (0, 0, i, 0))
    return pl.pallas_call(
        update_kernel,
        grid=(rows // step,),
        in_specs=[pl.BlockSpec(memory_space=pltpu.SMEM), moved_spec, moved_spec, flat_spec],
        out_specs=[flat_spec] * 3,
        out_shape=[jax.ShapeDtypeStruct(gradients.shape, jnp.float32)] * 3,
    )(clip_factor, zero, one, gradients)


def shift(array, key, devices):
    if key == 0:
        return array
    return lax.ppermute(array, AXES, [(i, i ^ key) for i in range(devices)])


def move_joint(zero, one, keys, devices):
    def branch(key_zero, key_one, arrays):
        return (shift(arrays[0], key_zero, devices), shift(arrays[1], key_one, devices))

    branches = [functools.partial(branch, i // devices, i % devices) for i in range(devices * devices)]
    return lax.switch(keys[0] * devices + keys[1], branches, (zero, one))


def move_each(zero, one, keys, devices):
    branches = [functools.partial(shift, key=i, devices=devices) for i in range(devices)]
    return (lax.switch(keys[0], branches, zero), lax.switch(keys[1], branches, one))


def sum_over_devices(value, devices):
    apart = 1
    while apart < devices:
        value = value + lax.ppermute(value, AXES, [(i, i ^ apart) for i in range(devices)])
        apart *= 2
    return value


def shards(old_params, old_first, old_second, gradients, old_table, new_table):
    tensors, halves, width = old_params.shape
    devices = lax.axis_size(AXES)
    rows = width // LANES
    old_key = old_table[:, 0]
    keys = jnp.bitwise_xor(jnp.right_shift(old_key, 1), new_table[:, 0])
    low_bits = jnp.bitwise_and(old_key, 1)

    def paired(array):
        return array.reshape(tensors, halves, rows, LANES).transpose(0, 2, 1, 3)

    flat = gradients.reshape(tensors, halves, rows, LANES)
    zero, one, squares = pack(low_bits, paired(old_params), paired(old_first), paired(old_second), flat)
    total_squares = sum_over_devices(jnp.sum(squares), devices)
    limit = jnp.float32(0.5 * math.sqrt(gradients.size * devices))
    clip_factor = limit / jnp.maximum(jnp.sqrt(total_squares), limit)
    move = move_joint if devices <= JOINT_DEVICES else move_each
    zero, one = move(zero, one, keys, devices)
    results = update(clip_factor.reshape(1), zero, one, flat)
    return tuple(result.reshape(gradients.shape) for result in results)


def solution(mesh):
    spec = P(None, AXES, None)
    return jax.shard_map(
        shards,
        mesh=mesh,
        in_specs=(spec, spec, spec, spec, P(), P()),
        out_specs=(spec, spec, spec),
        check_vma=False,
    )
```
